32 devices in a mesh: tensor: 2 (over x), batch: 4 (over y, core), context: 4 (over z).
Axes of the slice: x: 2, y: 2, z: 4, core: 2. Of those that a mesh axis runs over, the one named last changes fastest.
Arguments:
- block_input: bfloat16 [4, 1024, 2048], P('batch', 'context'), may hold values from -6 to 6
- gain_first: float32 [2048], replicated, may hold values from 0.1 to 1.9
- shift_first: float32 [2048], replicated, may hold values from -3 to 3
- attend_weight: bfloat16 [2048, 3, 2048], P(None, None, 'tensor'), may hold values from -0.125 to 0.125
- attend_offset: float32 [2, 2048], P(None, 'tensor'), may hold values from -1 to 1
- merge_weight: bfloat16 [2048, 2048], P('tensor'), may hold values from -1.5 to 1.5
- merge_offset: float32 [2048], replicated, may hold values from -3 to 3
- gain_second: float32 [2048], replicated, may hold values from 0.1 to 1.9
- shift_second: float32 [2048], replicated, may hold values from -3 to 3
- expand_weight: bfloat16 [2048, 8192], P(None, 'tensor'), may hold values from -0.125 to 0.125
- expand_offset: float32 [8192], P('tensor'), may hold values from -3 to 3
- reduce_weight: bfloat16 [8192, 2048], P('tensor'), may hold values from -0.0625 to 0.0625
- reduce_offset: float32 [2048], replicated, may hold values from -3 to 3
- key_mask: int32 [4, 1024], P('batch', 'context'), may hold values 0 or 1
- true_lengths: int32 [4], P('batch'), may hold values from 512 to 1024, as said below
- output_cotangent: bfloat16 [4, 1024, 2048], P('batch', 'context'), may hold values from -6 to 6
Outputs:
- block_output: bfloat16 [4, 1024, 2048], P('batch', 'context')
- input_gradient: bfloat16 [4, 1024, 2048], P('batch', 'context')
- gain_first_gradient: float32 [2048], replicated
- shift_first_gradient: float32 [2048], replicated
- attend_weight_gradient: float32 [2048, 3, 2048], P(('batch', 'context'), None, 'tensor')
- attend_offset_gradient: float32 [2, 2048], P(None, 'tensor')
- merge_weight_gradient: float32 [2048, 2048], P('tensor', ('batch', 'context'))
- merge_offset_gradient: float32 [2048], replicated
- gain_second_gradient: float32 [2048], replicated
- shift_second_gradient: float32 [2048], replicated
- expand_weight_gradient: float32 [2048, 8192], P(('batch', 'context'), 'tensor')
- expand_offset_gradient: float32 [8192], P('tensor')
- reduce_weight_gradient: float32 [8192, 2048], P('tensor', ('batch', 'context'))
- reduce_offset_gradient: float32 [2048], replicated
The draws below stay inside these ranges and needn't reach their ends.
Inputs may be any that keep to these rules, and one draw needn't show every extreme that they name: `true_lengths`: rows at or past a sequence's true length are padding; some sequence fills all 1024 slots in every draw.
All inputs are finite; a program needn't handle non-finite values. No bound on the sum of `key_mask` on one device may be relied on, other than what follows from the above.
Results may differ from the reference program's by a relative error of at most 0.02.
Values may be sent and summed in bfloat16 or wider, within the bound.
A program may use at most 256 MiB of HBM per device.

```python
import jax
import jax.numpy as jnp
from jax import lax

D = 2048
HEADS = 16
HEAD_DIM = 128
FF = 8192
LEN = 1024
SEQS = 4


def draw_true_lengths(key, part):
    drawn = jax.random.randint(key, (SEQS,), LEN // 2, LEN + 1)
    return drawn.at[0].set(LEN).astype(jnp.int32)


def touch_ends(array, stream_key, smallest, top_value):
    index_at = [jax.random.randint(jax.random.fold_in(stream_key, axis), (), 0, length) for axis, length in enumerate(array.shape)]
    widest = array.shape.index(max(array.shape))
    neighbour = index_at[:widest] + [(index_at[widest] + 1) % array.shape[widest]] + index_at[widest + 1:]
    return array.at[tuple(index_at)].set(smallest).at[tuple(neighbour)].set(top_value)


def raised(values, key, source, target, shards_of, factor):
    def block_of(axis_at):
        return (jnp.arange(values.shape[axis_at]) // (values.shape[axis_at] // shards_of)).reshape((-1,) + (1,) * (values.ndim - 1 - axis_at))

    near = jax.random.permutation(key, shards_of)[block_of(target)]
    other_side = (block_of(target) + shards_of // 2) % shards_of
    return jnp.where((block_of(source) == near) | (block_of(source) == other_side), factor * values, values)


def levels(own_key, extent, split, least, high):
    def one(dim, shards_of):
        steps = jax.random.uniform(jax.random.fold_in(jax.random.fold_in(own_key, 6), dim), (shards_of,), jnp.float32, least / len(split), high / len(split))
        return jnp.repeat(jnp.exp(steps), extent[dim] // shards_of).reshape((-1,) + (1,) * (len(extent) - dim - 1))

    factor_of = one(*split[0])
    for cut in split[1:]:
        factor_of = factor_of * one(*cut)
    return factor_of


def noise(stream_key, shape, scale, bound, shards=(), kind=jnp.bfloat16):
    array = scale * jax.random.normal(stream_key, shape, jnp.float32)
    if shards:
        array = array * levels(stream_key, shape, shards, -0.22, 0.18)
    return jnp.clip(array, -bound, bound).astype(kind)


def gaussian_with(key, extent, scale, bound, split, heavy, kind=jnp.bfloat16):
    array = scale * jax.random.normal(key, extent, jnp.float32)
    if split:
        array = array * levels(key, extent, split, -0.22, 0.18)
    return jnp.clip(raised(array, jax.random.fold_in(key, 3), *heavy), -bound, bound).astype(kind)


def setup_inputs(seed: int = 0) -> dict:
    keys = jax.random.split(jax.random.key(seed), 17)
    return {
        "block_input": noise(keys[0], (SEQS, LEN, D), 1.0, 6.0, ((0, 4), (1, 4))),
        "gain_first": jnp.clip(1.0 + 0.18 * jax.random.normal(keys[1], (D,), jnp.float32), 0.1, 1.9),
        "shift_first": noise(keys[2], (D,), 0.3, 3.0, (), jnp.float32),
        "attend_weight": noise(keys[3], (D, 3, HEADS * HEAD_DIM), D ** -0.5, 0.125, ((2, 2),)),
        "attend_offset": noise(keys[4], (2, HEADS * HEAD_DIM), 0.1, 1.0, ((1, 2),), jnp.float32),
        "merge_weight": noise(keys[5], (HEADS * HEAD_DIM, D), (max(HEADS * HEAD_DIM // 128, 1)) ** -0.5, 1.5, ((0, 2),)),
        "merge_offset": noise(keys[6], (D,), 0.3, 3.0, (), jnp.float32),
        "gain_second": jnp.clip(1.0 + 0.18 * jax.random.normal(keys[7], (D,), jnp.float32), 0.1, 1.9),
        "shift_second": noise(keys[8], (D,), 0.3, 3.0, (), jnp.float32),
        "expand_weight": noise(keys[9], (D, FF), D ** -0.5, 0.125, ((1, 2),)),
        "expand_offset": noise(keys[10], (FF,), 0.5, 3.0, ((0, 2),), jnp.float32),
        "reduce_weight": noise(keys[11], (FF, D), FF ** -0.5, 0.0625, ((0, 2),)),
        "reduce_offset": noise(keys[12], (D,), 0.3, 3.0, (), jnp.float32),
        "key_mask": touch_ends((jax.random.randint(keys[13], (SEQS, LEN), 0, 8) < 7).astype(jnp.int32), jax.random.fold_in(keys[13], 1), 0, 1),
        "true_lengths": draw_true_lengths(jax.random.fold_in(keys[16], 71), 0),
        "output_cotangent": gaussian_with(keys[15], (SEQS, LEN, D), 1.0, 6.0, ((0, 4), (1, 4)), (1, 2, 4, 2.0)),
    }


EPS = 1e-05
NEGATIVE = -1e+30
HIGHEST = lax.Precision.HIGHEST

@jax.custom_vjp
def low(v):
    return lax.optimization_barrier(v.astype(jnp.bfloat16)).astype(jnp.float32)

@jax.custom_vjp
def low_back(v):
    return v

def low_keep(v):
    return (low(v), None)

def low_pass(kept, grad):
    return (grad,)

def back_keep(v):
    return (v, None)

def back_low(kept, grad):
    return (low(grad),)
low.defvjp(low_keep, low_pass)
low_back.defvjp(back_keep, back_low)

def layer_norm(values, gain, shift):
    average = lax.optimization_barrier(jnp.mean(values, -1, keepdims=True))
    center = values - average
    spread = lax.optimization_barrier(jnp.mean(center * center, -1, keepdims=True))
    return center * lax.rsqrt(spread + EPS) * gain + shift

def forward(inputs, length_one, mask_one, gain_first, shift_first, attend_weight, attend_offset, merge_weight, merge_offset, gain_second, shift_second, expand_weight, expand_offset, reduce_weight, reduce_offset):
    normed = low(layer_norm(inputs, gain_first, shift_first))
    triple = jnp.einsum('td,dch->cth', normed, attend_weight, precision=HIGHEST)
    queries = low(low_back(triple[0] + attend_offset[0])).reshape(LEN, HEADS, HEAD_DIM)
    keys_all = low(low_back(triple[1])).reshape(LEN, HEADS, HEAD_DIM)
    values_all = low(low_back(triple[2] + attend_offset[1])).reshape(LEN, HEADS, HEAD_DIM)
    scores = low_back(jnp.einsum('qhe,khe->hqk', queries, keys_all, precision=HIGHEST) * HEAD_DIM ** (-0.5))
    position = jnp.arange(LEN, dtype=jnp.int32)
    key_live = (mask_one == 1) & (position < length_one)
    allowed = (position[None, :] <= position[:, None]) & (key_live[None, :] | (position[None, :] == position[:, None]))
    scores = jnp.where(allowed[None], scores, NEGATIVE)
    weights = low(jax.nn.softmax(scores, axis=-1))
    mixed = jnp.einsum('hqk,khe->qhe', weights, values_all, precision=HIGHEST).reshape(LEN, HEADS * HEAD_DIM)
    mixed = low(low_back(mixed))
    attended = low_back(jnp.dot(mixed, merge_weight, precision=HIGHEST)) + merge_offset
    middle = inputs + attended
    normed_two = low(layer_norm(middle, gain_second, shift_second))
    hidden = low_back(jnp.dot(normed_two, expand_weight, precision=HIGHEST) + expand_offset)
    active = low(jax.nn.gelu(hidden, approximate=True))
    return middle + jnp.dot(active, reduce_weight, precision=HIGHEST) + reduce_offset

def reference(block_input, gain_first, shift_first, attend_weight, attend_offset, merge_weight, merge_offset, gain_second, shift_second, expand_weight, expand_offset, reduce_weight, reduce_offset, key_mask, true_lengths, output_cotangent):
    params = tuple((member.astype(jnp.float32) for member in (gain_first, shift_first, attend_weight, attend_offset, merge_weight, merge_offset, gain_second, shift_second, expand_weight, expand_offset, reduce_weight, reduce_offset)))

    def one_sequence(totals, pieces):
        inputs, mask_one, length_one, cotangent = pieces

        def apply(inputs_float, *weights_list):
            return forward(inputs_float, length_one, mask_one, *weights_list)
        result, pullback = jax.vjp(apply, inputs.astype(jnp.float32), *params)
        position = jnp.arange(LEN, dtype=jnp.int32)
        live_rows = (position < length_one).astype(jnp.float32)
        gradients = pullback(cotangent.astype(jnp.float32) * live_rows[:, None])
        totals = jax.tree.map(lambda running, update: running + update, totals, tuple(gradients[1:]))
        return (totals, (result.astype(jnp.bfloat16), gradients[0].astype(jnp.bfloat16)))
    zeros = tuple((jnp.zeros_like(member) for member in params))
    totals, (outputs, input_grads) = lax.scan(one_sequence, zeros, (block_input, key_mask, true_lengths, output_cotangent))
    return (outputs, input_grads, totals[0], totals[1], totals[2], totals[3], totals[4], totals[5], totals[6], totals[7], totals[8], totals[9], totals[10], totals[11])
```

```python
import functools

import jax
import jax.numpy as jnp
from jax import lax
from jax.experimental import pallas as pl
from jax.experimental.pallas import tpu as pltpu
from jax.sharding import PartitionSpec as P

HEAD_DIM = 128


EPS = 1e-05
NEGATIVE = -1e30


def norm_parts(values, gain, shift):
    average = jnp.mean(values, -1, keepdims=True)
    center = values - average
    inverse = lax.rsqrt(jnp.mean(center * center, -1, keepdims=True) + EPS)
    normal = center * inverse
    return (normal * gain + shift, normal, inverse)


def norm_back(upstream, normal, inverse, gain):
    gain_part = jnp.sum(upstream * normal, (0, 1))
    shift_part = jnp.sum(upstream, (0, 1))
    scaled = upstream * gain
    inner = (
        scaled
        - jnp.mean(scaled, -1, keepdims=True)
        - normal * jnp.mean(scaled * normal, -1, keepdims=True)
    )
    return (inverse * inner, gain_part, shift_part)


def allowed_mask(query_pos, key_pos, key_flags):
    causal = key_pos[None, :] <= query_pos[:, None]
    itself = key_pos[None, :] == query_pos[:, None]
    return causal[None, None] & ((key_flags[:, None, None, :] > 0.5) | itself[None, None])


def masked_scores(query_heads, key_heads, allowed, scale):
    raw = (
        jnp.einsum("sqhe,skhe->shqk", query_heads, key_heads, preferred_element_type=jnp.float32)
        * scale
    )
    return jnp.where(allowed, raw, NEGATIVE)


def gelu_tanh(values):
    return jax.nn.gelu(values, approximate=True)


def tensor_total(values):
    return lax.psum(values.astype(jnp.bfloat16), "tensor").astype(jnp.float32)


def general(
    block_input,
    gain_first,
    shift_first,
    attend_weight,
    attend_offset,
    merge_weight,
    merge_offset,
    gain_second,
    shift_second,
    expand_weight,
    expand_offset,
    reduce_weight,
    reduce_offset,
    key_mask,
    true_lengths,
    output_cotangent,
):
    seq_count, block_len, width = block_input.shape
    local_width = attend_weight.shape[2]
    head_size = HEAD_DIM
    local_heads = local_width // head_size
    scale = head_size ** (-0.5)
    full_len = block_len * lax.axis_size("context")
    query_pos = lax.axis_index("context") * block_len + jnp.arange(block_len, dtype=jnp.int32)
    key_pos = jnp.arange(full_len, dtype=jnp.int32)

    def heads_of(values):
        return values.reshape(values.shape[0], values.shape[1], local_heads, head_size)

    inputs = block_input.astype(jnp.float32)
    normed, normal_one, inverse_one = norm_parts(inputs, gain_first, shift_first)
    normed = normed.astype(jnp.bfloat16)
    triple = jnp.einsum("std,dch->csth", normed, attend_weight, preferred_element_type=jnp.float32)
    queries = (triple[0] + attend_offset[0]).astype(jnp.bfloat16)
    keys_own = triple[1].astype(jnp.bfloat16)
    values_own = (triple[2] + attend_offset[1]).astype(jnp.bfloat16)
    row_live = query_pos[None, :] < true_lengths[:, None]
    key_flags = ((key_mask == 1) & row_live).astype(jnp.bfloat16)
    keys_all, values_all, flags_all = (
        lax.all_gather(keys_own, "context", axis=1, tiled=True),
        lax.all_gather(values_own, "context", axis=1, tiled=True),
        lax.all_gather(key_flags, "context", axis=1, tiled=True),
    )
    query_heads = heads_of(queries)
    key_heads = heads_of(keys_all)
    value_heads = heads_of(values_all)
    allowed = allowed_mask(query_pos, key_pos, flags_all)
    scores = masked_scores(query_heads, key_heads, allowed, scale)
    top_score = jnp.max(scores, -1, keepdims=True)
    log_total = top_score + jnp.log(jnp.sum(jnp.exp(scores - top_score), -1, keepdims=True))
    weights = jnp.exp(scores - log_total)
    weights_low = weights.astype(jnp.bfloat16)
    mixed = jnp.einsum(
        "shqk,skhe->sqhe", weights_low, value_heads, preferred_element_type=jnp.float32
    )
    mixed = mixed.reshape(seq_count, block_len, local_width).astype(jnp.bfloat16)
    attended_part = jnp.einsum(
        "sth,hd->std", mixed, merge_weight, preferred_element_type=jnp.float32
    )
    middle = inputs + tensor_total(attended_part) + merge_offset
    normed_two, normal_two, inverse_two = norm_parts(middle, gain_second, shift_second)
    normed_two = normed_two.astype(jnp.bfloat16)
    hidden = (
        jnp.einsum("std,df->stf", normed_two, expand_weight, preferred_element_type=jnp.float32)
        + expand_offset
    )
    active, gelu_back = jax.vjp(gelu_tanh, hidden)
    active_low = active.astype(jnp.bfloat16)
    reduced_part = jnp.einsum(
        "stf,fd->std", active_low, reduce_weight, preferred_element_type=jnp.float32
    )
    block_output = (middle + tensor_total(reduced_part) + reduce_offset).astype(jnp.bfloat16)
    upstream = output_cotangent.astype(jnp.float32) * row_live.astype(jnp.float32)[:, :, None]
    upstream_low = upstream.astype(jnp.bfloat16)
    reduce_grad = jnp.einsum(
        "stf,std->fd", active_low, upstream_low, preferred_element_type=jnp.float32
    )
    reduce_off_grad = jnp.sum(upstream, (0, 1))
    active_grad = jnp.einsum(
        "std,fd->stf", upstream_low, reduce_weight, preferred_element_type=jnp.float32
    )
    hidden_grad = gelu_back(active_grad)[0].astype(jnp.bfloat16)
    expand_off_grad = jnp.sum(hidden_grad.astype(jnp.float32), (0, 1))
    expand_grad = jnp.einsum(
        "std,stf->df", normed_two, hidden_grad, preferred_element_type=jnp.float32
    )
    second_part = jnp.einsum(
        "stf,df->std", hidden_grad, expand_weight, preferred_element_type=jnp.float32
    )
    middle_part, gain_two_grad, shift_two_grad = norm_back(
        tensor_total(second_part), normal_two, inverse_two, gain_second
    )
    middle_grad = upstream + middle_part
    middle_low = middle_grad.astype(jnp.bfloat16)
    merge_off_grad = jnp.sum(middle_grad, (0, 1))
    merge_grad = jnp.einsum("sth,std->hd", mixed, middle_low, preferred_element_type=jnp.float32)
    mixed_grad = jnp.einsum(
        "std,hd->sth", middle_low, merge_weight, preferred_element_type=jnp.float32
    ).astype(jnp.bfloat16)
    mixed_heads = heads_of(mixed_grad)
    scores = masked_scores(query_heads, key_heads, allowed, scale)
    weights = jnp.exp(scores - log_total)
    weights_grad = jnp.einsum(
        "sqhe,skhe->shqk", mixed_heads, value_heads, preferred_element_type=jnp.float32
    )
    row_dot = jnp.sum(weights * weights_grad, -1, keepdims=True)
    score_grad = (weights * (weights_grad - row_dot)).astype(jnp.bfloat16)
    query_grad = (
        jnp.einsum("shqk,skhe->sqhe", score_grad, key_heads, preferred_element_type=jnp.float32)
        * scale
    )
    query_grad = query_grad.reshape(seq_count, block_len, local_width).astype(jnp.bfloat16)
    key_part = (
        jnp.einsum("shqk,sqhe->skhe", score_grad, query_heads, preferred_element_type=jnp.float32)
        * scale
    )
    value_part = jnp.einsum(
        "shqk,sqhe->skhe",
        weights.astype(jnp.bfloat16),
        mixed_heads,
        preferred_element_type=jnp.float32,
    )
    key_sum, value_sum = (
        lax.psum_scatter(
            key_part.reshape(seq_count, full_len, local_width).astype(jnp.bfloat16),
            "context",
            scatter_dimension=1,
            tiled=True,
        ).astype(jnp.float32),
        lax.psum_scatter(
            value_part.reshape(seq_count, full_len, local_width).astype(jnp.bfloat16),
            "context",
            scatter_dimension=1,
            tiled=True,
        ).astype(jnp.float32),
    )
    key_low = key_sum.astype(jnp.bfloat16)
    value_low = value_sum.astype(jnp.bfloat16)
    offset_grad = jnp.stack(
        [
            jnp.sum(query_grad.astype(jnp.float32), (0, 1)),
            jnp.sum(value_low.astype(jnp.float32), (0, 1)),
        ]
    )
    triple_grad = jnp.stack([query_grad, key_low, value_low])
    attend_grad = jnp.einsum(
        "std,csth->dch", normed, triple_grad, preferred_element_type=jnp.float32
    )
    first_part = jnp.einsum(
        "csth,dch->std", triple_grad, attend_weight, preferred_element_type=jnp.float32
    )
    input_part, gain_one_grad, shift_one_grad = norm_back(
        tensor_total(first_part), normal_one, inverse_one, gain_first
    )
    input_gradient = (middle_grad + input_part).astype(jnp.bfloat16)
    attend_total, expand_total = (
        lax.psum_scatter(
            attend_grad.astype(jnp.bfloat16), ("batch", "context"), scatter_dimension=0, tiled=True
        ).astype(jnp.float32),
        lax.psum_scatter(
            expand_grad.astype(jnp.bfloat16), ("batch", "context"), scatter_dimension=0, tiled=True
        ).astype(jnp.float32),
    )
    merge_total, reduce_total = (
        lax.psum_scatter(
            merge_grad.astype(jnp.bfloat16), ("batch", "context"), scatter_dimension=1, tiled=True
        ).astype(jnp.float32),
        lax.psum_scatter(
            reduce_grad.astype(jnp.bfloat16), ("batch", "context"), scatter_dimension=1, tiled=True
        ).astype(jnp.float32),
    )
    smalls = (
        lax.psum(gain_one_grad.astype(jnp.bfloat16), ("batch", "context")).astype(jnp.float32),
        lax.psum(shift_one_grad.astype(jnp.bfloat16), ("batch", "context")).astype(jnp.float32),
        lax.psum(offset_grad.astype(jnp.bfloat16), ("batch", "context")).astype(jnp.float32),
        lax.psum(merge_off_grad.astype(jnp.bfloat16), ("batch", "context")).astype(jnp.float32),
        lax.psum(gain_two_grad.astype(jnp.bfloat16), ("batch", "context")).astype(jnp.float32),
        lax.psum(shift_two_grad.astype(jnp.bfloat16), ("batch", "context")).astype(jnp.float32),
        lax.psum(expand_off_grad.astype(jnp.bfloat16), ("batch", "context")).astype(jnp.float32),
        lax.psum(reduce_off_grad.astype(jnp.bfloat16), ("batch", "context")).astype(jnp.float32),
    )
    return (
        block_output,
        input_gradient,
        smalls[0],
        smalls[1],
        attend_total,
        smalls[2],
        merge_total,
        smalls[3],
        smalls[4],
        smalls[5],
        expand_total,
        smalls[6],
        reduce_total,
        smalls[7],
    )


MESH = pl.DeviceIdType.MESH
F32 = jnp.float32
BF16 = jnp.bfloat16
VMEM_WHOLE = pl.BlockSpec(memory_space=pltpu.VMEM)
TILE = 512


def mm(left, right):
    return lax.dot_general(left, right, (((1,), (0,)), ((), ())), preferred_element_type=F32)


def mm_nt(left, right):
    return lax.dot_general(left, right, (((1,), (1,)), ((), ())), preferred_element_type=F32)


def mm_tn(left, right):
    return lax.dot_general(left, right, (((0,), (0,)), ((), ())), preferred_element_type=F32)


def whole(shape):
    return pl.BlockSpec(shape, lambda *ids: (0,) * len(shape))


def call(body, grid, ins, outs, operands, scratch=(), flops=0, moved=0, name=None):
    in_specs = [spec for spec in ins]
    return pl.pallas_call(
        body,
        grid_spec=pltpu.PrefetchScalarGridSpec(
            num_scalar_prefetch=1,
            grid=grid,
            in_specs=in_specs,
            out_specs=[spec for spec, _ in outs],
            scratch_shapes=list(scratch),
        ),
        out_shape=[shape for _, shape in outs],
        cost_estimate=pl.CostEstimate(flops=flops, bytes_accessed=moved, transcendentals=0),
        name=name,
    )(*operands)


def sds(shape, kind):
    return jax.ShapeDtypeStruct(shape, kind)


def norm_rows(values):
    average = jnp.mean(values, -1, keepdims=True)
    center = values - average
    inverse = lax.rsqrt(jnp.mean(center * center, -1, keepdims=True) + EPS)
    return center * inverse, inverse


def qkv_body(pos, x_ref, gain_ref, shift_ref, w_ref, off_ref, out_ref, normed_ref):
    part = pl.program_id(0)

    @pl.when((part == 0) & (pl.program_id(1) == 0))
    def _():
        normal, _ = norm_rows(x_ref[...].astype(F32))
        normed_ref[...] = (normal * gain_ref[...] + shift_ref[...]).astype(BF16)

    bias = jnp.where(part == 0, off_ref[0:1, :], jnp.where(part == 2, off_ref[1:2, :], 0.0))
    out_ref[...] = (mm(normed_ref[...], w_ref[...]) + bias).astype(BF16)


def qkv_call(pos, x, gain, shift, weight, offset):
    rows, depth = x.shape
    width = weight.shape[2]
    return call(
        qkv_body,
        (3, width // TILE),
        [
            whole((rows, depth)),
            whole((1, depth)),
            whole((1, depth)),
            pl.BlockSpec((None, depth, TILE), lambda c, n, pos: (c, 0, n)),
            pl.BlockSpec((2, TILE), lambda c, n, pos: (0, n)),
        ],
        [
            (pl.BlockSpec((None, rows, TILE), lambda c, n, pos: (c, 0, n)), sds((3, rows, width), BF16)),
            (whole((rows, depth)), sds((rows, depth), BF16)),
        ],
        (pos, x, gain, shift, weight, offset),
        flops=2 * rows * depth * 3 * width,
        moved=2 * depth * 3 * width,
        name="qkv",
    )


def greet(peers):
    barrier = pltpu.get_barrier_semaphore()
    for peer in peers:
        pl.semaphore_signal(barrier, inc=1, device_id=peer, device_id_type=MESH)
    pl.semaphore_wait(barrier, len(peers))


def spread_body(n, parts, with_flags, *refs):
    if with_flags:
        src, flags, dst, all_flags, send, recv, fsend, frecv = refs
    else:
        src, dst, send, recv = refs
    me = lax.axis_index("context")
    rows = src.shape[1]
    cols = src.shape[2] // n
    greet([{"context": lax.rem(me + r, n)} for r in range(1, n)])
    mine = pl.ds(pl.multiple_of(me * rows, rows), rows)
    copies = []
    for c in range(parts):
        for r in range(1, n):
            to = lax.rem(me + r, n)
            copies.append(
                pltpu.make_async_remote_copy(
                    src_ref=src.at[c, :, pl.ds(pl.multiple_of(to * cols, cols), cols)],
                    dst_ref=dst.at[c, mine, :],
                    send_sem=send.at[c, r - 1],
                    recv_sem=recv.at[c, r - 1],
                    device_id={"context": to},
                    device_id_type=MESH,
                )
            )
    if with_flags:
        for r in range(1, n):
            copies.append(
                pltpu.make_async_remote_copy(
                    src_ref=flags,
                    dst_ref=all_flags.at[me],
                    send_sem=fsend.at[r - 1],
                    recv_sem=frecv.at[r - 1],
                    device_id={"context": lax.rem(me + r, n)},
                    device_id_type=MESH,
                )
            )
    for copy in copies:
        copy.start()
    for c in range(parts):
        dst[c, mine, :] = src[c, :, pl.ds(pl.multiple_of(me * cols, cols), cols)]
    if with_flags:
        all_flags[me] = flags[...]
    for copy in copies:
        copy.wait()


def spread(n, src, flags, collective):
    parts, rows, width = src.shape
    with_flags = flags is not None
    outs = [sds((parts, n * rows, width // n), BF16)]
    scratch = [pltpu.SemaphoreType.DMA((parts, n - 1))] * 2
    if with_flags:
        outs.append(sds((n, *flags.shape), flags.dtype))
        scratch += [pltpu.SemaphoreType.DMA((n - 1,))] * 2
    return pl.pallas_call(
        functools.partial(spread_body, n, parts, with_flags),
        out_shape=outs,
        in_specs=[VMEM_WHOLE] * (1 + with_flags),
        out_specs=[VMEM_WHOLE] * len(outs),
        scratch_shapes=scratch,
        compiler_params=pltpu.CompilerParams(collective_id=collective, has_side_effects=True),
        name=f"spread{collective}",
    )(*((src, flags) if with_flags else (src,)))


def collect_body(n, parts, src, dst, send, recv):
    me = lax.axis_index("context")
    rows = src.shape[1] // n
    cols = src.shape[2]
    greet([{"context": lax.rem(me + r, n)} for r in range(1, n)])
    mine = pl.ds(pl.multiple_of(me * cols, cols), cols)
    copies = []
    for c in range(parts):
        for r in range(1, n):
            to = lax.rem(me + r, n)
            copies.append(
                pltpu.make_async_remote_copy(
                    src_ref=src.at[c, pl.ds(pl.multiple_of(to * rows, rows), rows), :],
                    dst_ref=dst.at[c, :, mine],
                    send_sem=send.at[c, r - 1],
                    recv_sem=recv.at[c, r - 1],
                    device_id={"context": to},
                    device_id_type=MESH,
                )
            )
    for copy in copies:
        copy.start()
    for c in range(parts):
        dst[c, :, mine] = src[c, pl.ds(pl.multiple_of(me * rows, rows), rows), :]
    for copy in copies:
        copy.wait()


def collect(n, src, collective):
    parts, rows, width = src.shape
    return pl.pallas_call(
        functools.partial(collect_body, n, parts),
        out_shape=sds((parts, rows // n, width * n), BF16),
        in_specs=[VMEM_WHOLE],
        out_specs=VMEM_WHOLE,
        scratch_shapes=[pltpu.SemaphoreType.DMA((parts, n - 1))] * 2,
        compiler_params=pltpu.CompilerParams(collective_id=collective, has_side_effects=True),
        name=f"collect{collective}",
    )(src)


def mixed_body(n, src, dst, own, send, recv, xsend, xrecv):
    me = lax.axis_index("context")
    side = lax.axis_index("tensor")
    rows = src.shape[0] // n
    cols = src.shape[1]
    width = n * cols
    greet([{"context": lax.rem(me + r, n)} for r in range(1, n)] + [{"tensor": 1 - side}])

    def place(origin):
        return dst.at[:, pl.ds(pl.multiple_of(side * width + origin * cols, cols), cols)]

    copies = []
    for r in range(1, n):
        to = lax.rem(me + r, n)
        copies.append(
            pltpu.make_async_remote_copy(
                src_ref=src.at[pl.ds(pl.multiple_of(to * rows, rows), rows), :],
                dst_ref=place(me),
                send_sem=send.at[r - 1],
                recv_sem=recv.at[r - 1],
                device_id={"context": to},
                device_id_type=MESH,
            )
        )
    for copy in copies:
        copy.start()
    across = []
    for r in range(n):
        origin = lax.rem(me + n - r, n)
        if r:
            copies[r - 1].wait()
            source = place(origin)
        else:
            source = src.at[pl.ds(pl.multiple_of(me * rows, rows), rows), :]
        copy = pltpu.make_async_remote_copy(
            src_ref=source,
            dst_ref=place(origin),
            send_sem=xsend.at[r],
            recv_sem=xrecv.at[r],
            device_id={"tensor": 1 - side},
            device_id_type=MESH,
        )
        copy.start()
        across.append(copy)
        if not r:
            here = pl.ds(pl.multiple_of(side * width + me * cols, cols), cols)
            dst[:, here] = src[pl.ds(pl.multiple_of(me * rows, rows), rows), :]
    own[...] = dst[:, pl.ds(pl.multiple_of(side * width, width), width)]
    for copy in across:
        copy.wait()


def mixed_call(n, src, collective):
    rows, cols = src.shape
    return pl.pallas_call(
        functools.partial(mixed_body, n),
        out_shape=[sds((rows // n, 2 * n * cols), BF16), sds((rows // n, n * cols), BF16)],
        in_specs=[VMEM_WHOLE],
        out_specs=[VMEM_WHOLE] * 2,
        scratch_shapes=[pltpu.SemaphoreType.DMA((n - 1,))] * 2 + [pltpu.SemaphoreType.DMA((n,))] * 2,
        compiler_params=pltpu.CompilerParams(collective_id=collective, has_side_effects=True),
        name="mixed_exchange",
    )(src)


def allowed_block(row, size, count, flags):
    query = row * size + lax.broadcasted_iota(jnp.int32, (size, count), 0)
    key = lax.broadcasted_iota(jnp.int32, (size, count), 1)
    return (key <= query) & ((flags[:, :count] > 0.5) | (key == query))


def key_row(flag_ref):
    return jnp.concatenate([flag_ref[j, 0:1, :] for j in range(flag_ref.shape[0])], axis=1)


def attend_body(n, pos, qkv_ref, flag_ref, mixed_ref, lse_ref):
    size = qkv_ref.shape[1] // n
    scale = HEAD_DIM ** (-0.5)
    flags = key_row(flag_ref)
    for row in range(n):
        count = size * (row + 1)
        rows = slice(row * size, count)
        scores = mm_nt(qkv_ref[0, rows, :], qkv_ref[1, :count, :]) * scale
        scores = jnp.where(allowed_block(row, size, count, flags), scores, NEGATIVE)
        top = jnp.max(scores, -1, keepdims=True)
        total = top + jnp.log(jnp.sum(jnp.exp(scores - top), -1, keepdims=True))
        weights = jnp.exp(scores - total).astype(BF16)
        mixed_ref[rows, :] = mm(weights, qkv_ref[2, :count, :]).astype(BF16)
        lse_ref[rows, :] = jnp.broadcast_to(total, (size, HEAD_DIM))


def attend_call(n, pos, qkv, flags):
    _, full, width = qkv.shape
    heads = width // HEAD_DIM
    return call(
        functools.partial(attend_body, n),
        (heads,),
        [pl.BlockSpec((3, full, HEAD_DIM), lambda h, pos: (0, 0, h)), whole(flags.shape)],
        [
            (pl.BlockSpec((full, HEAD_DIM), lambda h, pos: (0, h)), sds((full, width), BF16)),
            (pl.BlockSpec((full, HEAD_DIM), lambda h, pos: (0, h)), sds((full, width), F32)),
        ],
        (pos, qkv, flags),
        flops=4 * full * full * width,
        moved=10 * full * width,
        name="attend",
    )


def attend_back_body(n, pos, qkv_ref, flag_ref, lse_ref, up_ref, out_ref, dk_ref, dv_ref):
    size = qkv_ref.shape[1] // n
    scale = HEAD_DIM ** (-0.5)
    flags = key_row(flag_ref)
    dk_ref[...] = jnp.zeros_like(dk_ref)
    dv_ref[...] = jnp.zeros_like(dv_ref)
    for row in range(n):
        count = size * (row + 1)
        rows = slice(row * size, count)
        query = qkv_ref[0, rows, :]
        up = up_ref[rows, :]
        scores = mm_nt(query, qkv_ref[1, :count, :]) * scale
        scores = jnp.where(allowed_block(row, size, count, flags), scores, NEGATIVE)
        weights = jnp.exp(scores - lse_ref[rows, 0:1])
        weights_grad = mm_nt(up, qkv_ref[2, :count, :])
        row_dot = jnp.sum(weights * weights_grad, -1, keepdims=True)
        score_grad = (weights * (weights_grad - row_dot)).astype(BF16)
        dv_ref[:count, :] += mm_tn(weights.astype(BF16), up)
        dk_ref[:count, :] += mm_tn(score_grad, query)
        out_ref[0, rows, :] = (mm(score_grad, qkv_ref[1, :count, :]) * scale).astype(BF16)
    out_ref[1] = (dk_ref[...] * scale).astype(BF16)
    out_ref[2] = dv_ref[...].astype(BF16)


def attend_back_call(n, pos, qkv, flags, lse, up):
    _, full, width = qkv.shape
    heads = width // HEAD_DIM
    return call(
        functools.partial(attend_back_body, n),
        (heads,),
        [
            pl.BlockSpec((3, full, HEAD_DIM), lambda h, pos: (0, 0, h)),
            whole(flags.shape),
            pl.BlockSpec((full, HEAD_DIM), lambda h, pos: (0, h)),
            pl.BlockSpec((full, HEAD_DIM), lambda h, pos: (0, h)),
        ],
        [(pl.BlockSpec((3, full, HEAD_DIM), lambda h, pos: (0, 0, h)), sds((3, full, width), BF16))],
        (pos, qkv, flags, lse, up),
        scratch=[pltpu.VMEM((full, HEAD_DIM), F32)] * 2,
        flops=10 * full * full * width,
        moved=20 * full * width,
        name="attend_back",
    )[0]


def merge_body(pos, x_ref, mixed_ref, own_ref, near_ref, far_ref, off_ref, gain_ref, shift_ref, middle_ref, normed_ref):
    step = pl.program_id(0)
    side, core = pos[0], lax.rem(pos[1], 2)
    half = near_ref.shape[0]
    tile = off_ref.shape[1]

    def piece(which, part, weight):
        start = pl.multiple_of(which * 2 * half + part * half, half)
        return mm(mixed_ref[:, pl.ds(start, half)], weight)

    own = piece(side, 0, own_ref[:half, :]) + piece(side, 1, own_ref[half:, :])
    other = piece(1 - side, core, near_ref[...]) + piece(1 - side, 1 - core, far_ref[...])
    columns = pl.ds(pl.multiple_of(step * tile, tile), tile)
    middle_ref[:, columns] = x_ref[...].astype(F32) + (own + other) + off_ref[...]

    @pl.when(step == pl.num_programs(0) - 1)
    def _():
        normal, _ = norm_rows(middle_ref[...])
        normed_ref[...] = (normal * gain_ref[...] + shift_ref[...]).astype(BF16)


def merge_call(pos, x, mixed, own, near, far, offset, gain, shift):
    rows, depth = x.shape
    half = near.shape[0]
    column = lambda n, pos: (0, n)
    return call(
        merge_body,
        (depth // TILE,),
        [
            pl.BlockSpec((rows, TILE), column),
            whole(mixed.shape),
            pl.BlockSpec((2 * half, TILE), column),
            pl.BlockSpec((half, TILE), column),
            pl.BlockSpec((half, TILE), column),
            pl.BlockSpec((1, TILE), column),
            whole((1, depth)),
            whole((1, depth)),
        ],
        [(whole((rows, depth)), sds((rows, depth), F32)), (whole((rows, depth)), sds((rows, depth), BF16))],
        (pos, x, mixed, own, near, far, offset, gain, shift),
        flops=2 * rows * depth * 4 * half,
        moved=8 * half * depth,
        name="merge",
    )


GELU_SCALE = 0.7978845608028654
GELU_CUBE = 0.044715


def expand_body(pos, normed_ref, w_ref, off_ref, up_ref, r_ref, active_ref, grad_ref, sum_ref):
    hidden = mm(normed_ref[...], w_ref[...]) + off_ref[...]
    square = hidden * hidden
    bend = jnp.tanh(GELU_SCALE * (hidden + GELU_CUBE * (square * hidden)))
    half = 0.5 * (1.0 + bend)
    active_ref[...] = (hidden * half).astype(BF16)
    slope = half + (0.5 * GELU_SCALE) * hidden * (1.0 - bend * bend) * (1.0 + (3.0 * GELU_CUBE) * square)
    grad = (mm_nt(up_ref[...], r_ref[...]) * slope).astype(BF16)
    grad_ref[...] = grad
    sum_ref[...] = jnp.sum(grad.astype(F32), 0, keepdims=True)


def expand_call(pos, part, parts, normed, weight, offset, up, reduce_weight):
    rows, depth = normed.shape
    width = weight.shape[1] // parts
    base = part * (width // TILE)
    return call(
        expand_body,
        (width // TILE,),
        [
            whole((rows, depth)),
            pl.BlockSpec((depth, TILE), lambda n, pos: (0, base + n)),
            pl.BlockSpec((1, TILE), lambda n, pos: (0, base + n)),
            whole((rows, depth)),
            pl.BlockSpec((TILE, depth), lambda n, pos: (base + n, 0)),
        ],
        [
            (pl.BlockSpec((rows, TILE), lambda n, pos: (0, n)), sds((rows, width), BF16)),
            (pl.BlockSpec((rows, TILE), lambda n, pos: (0, n)), sds((rows, width), BF16)),
            (pl.BlockSpec((1, TILE), lambda n, pos: (0, n)), sds((1, width), F32)),
        ],
        (pos, normed, weight, offset, up, reduce_weight),
        flops=4 * rows * depth * width,
        moved=4 * depth * width,
        name=f"expand{part}",
    )


def rows_body(count, pos, *refs):
    w_ref, out_ref = refs[count], refs[count + 1]
    start, total = 0, None
    for ref in refs[:count]:
        width = ref.shape[1]
        term = mm_nt(ref[...], w_ref[:, start : start + width])
        total = term if total is None else total + term
        start += width
    out_ref[...] = total.astype(BF16)


def rows_call(pos, pieces, weight, name):
    rows = pieces[0].shape[0]
    depth, width = weight.shape
    return call(
        functools.partial(rows_body, len(pieces)),
        (depth // TILE,),
        [whole(piece.shape) for piece in pieces] + [pl.BlockSpec((TILE, width), lambda n, pos: (n, 0))],
        [(pl.BlockSpec((rows, TILE), lambda n, pos: (0, n)), sds((rows, depth), BF16))],
        (pos, *pieces, weight),
        flops=2 * rows * depth * width,
        moved=2 * depth * width,
        name=name,
    )[0]


def columns_body(count, pos, *refs):
    w_ref, out_ref = refs[count], refs[count + 1]
    start, total = 0, None
    for ref in refs[:count]:
        width = ref.shape[1]
        term = mm(ref[...], w_ref[start : start + width, :])
        total = term if total is None else total + term
        start += width
    out_ref[...] = total.astype(BF16)


def columns_call(pos, pieces, weight, name):
    rows = pieces[0].shape[0]
    width, depth = weight.shape
    return call(
        functools.partial(columns_body, len(pieces)),
        (depth // TILE,),
        [whole(piece.shape) for piece in pieces] + [pl.BlockSpec((width, TILE), lambda n, pos: (0, n))],
        [(pl.BlockSpec((rows, TILE), lambda n, pos: (0, n)), sds((rows, depth), BF16))],
        (pos, *pieces, weight),
        flops=2 * rows * depth * width,
        moved=2 * depth * width,
        name=name,
    )[0]


def norm_back_rows(upstream, values, gain):
    normal, inverse = norm_rows(values)
    gain_part = jnp.sum(upstream * normal, 0, keepdims=True)
    shift_part = jnp.sum(upstream, 0, keepdims=True)
    scaled = upstream * gain
    inner = scaled - jnp.mean(scaled, -1, keepdims=True) - normal * jnp.mean(scaled * normal, -1, keepdims=True)
    return inverse * inner, gain_part, shift_part


def middle_back_body(pos, own_ref, peer_ref, middle_ref, gain_ref, up_ref, w_ref, out_ref, grad_ref, low_ref, gg_ref, sg_ref, mg_ref):
    @pl.when(pl.program_id(0) == 0)
    def _():
        upstream = own_ref[...].astype(F32) + peer_ref[...].astype(F32)
        part, gg_ref[...], sg_ref[...] = norm_back_rows(upstream, middle_ref[...], gain_ref[...])
        grad = up_ref[...].astype(F32) + part
        grad_ref[...] = grad
        low_ref[...] = grad.astype(BF16)
        mg_ref[...] = jnp.sum(grad, 0, keepdims=True)

    out_ref[...] = mm_nt(low_ref[...], w_ref[...]).astype(BF16)


def middle_back_call(pos, own, peer, middle, gain, up, weight):
    rows, depth = own.shape
    width = weight.shape[0]
    tile = TILE // 2
    full, line = whole((rows, depth)), whole((1, depth))
    return call(
        middle_back_body,
        (width // tile,),
        [full, full, full, line, full, pl.BlockSpec((tile, depth), lambda n, pos: (n, 0))],
        [
            (pl.BlockSpec((rows, tile), lambda n, pos: (0, n)), sds((rows, width), BF16)),
            (full, sds((rows, depth), F32)),
            (full, sds((rows, depth), BF16)),
            (line, sds((1, depth), F32)),
            (line, sds((1, depth), F32)),
            (line, sds((1, depth), F32)),
        ],
        (pos, own, peer, middle, gain, up, weight),
        flops=2 * rows * depth * width,
        moved=2 * depth * width,
        name="middle_back",
    )


def first_body(pos, grads_ref, w_ref, out_ref, sum_ref):
    @pl.when(pl.program_id(0) == 0)
    def _():
        sum_ref[0:1, :] = jnp.sum(grads_ref[0].astype(F32), 0, keepdims=True)
        sum_ref[1:2, :] = jnp.sum(grads_ref[2].astype(F32), 0, keepdims=True)

    total = mm_nt(grads_ref[0], w_ref[0]) + mm_nt(grads_ref[1], w_ref[1]) + mm_nt(grads_ref[2], w_ref[2])
    out_ref[...] = total.astype(BF16)


def first_call(pos, grads, weight):
    _, rows, width = grads.shape
    depth = weight.shape[1]
    return call(
        first_body,
        (depth // TILE,),
        [whole(grads.shape), pl.BlockSpec((3, TILE, width), lambda n, pos: (0, n, 0))],
        [
            (pl.BlockSpec((rows, TILE), lambda n, pos: (0, n)), sds((rows, depth), BF16)),
            (whole((2, width)), sds((2, width), F32)),
        ],
        (pos, grads, weight),
        flops=6 * rows * depth * width,
        moved=6 * depth * width,
        name="first_part",
    )


def input_back_body(own_ref, peer_ref, x_ref, gain_ref, grad_ref, out_ref, gg_ref, sg_ref):
    upstream = own_ref[...].astype(F32) + peer_ref[...].astype(F32)
    part, gg_ref[...], sg_ref[...] = norm_back_rows(upstream, x_ref[...].astype(F32), gain_ref[...])
    out_ref[...] = (grad_ref[...] + part).astype(BF16)


def input_back_call(own, peer, x, gain, grad):
    rows, depth = own.shape
    return pl.pallas_call(
        input_back_body,
        out_shape=[sds((rows, depth), BF16), sds((1, depth), F32), sds((1, depth), F32)],
        name="input_back",
    )(own, peer, x, gain, grad)


def weight_body(pos, *refs):
    out_ref = refs[-1]
    total = None
    for d_ref, t_ref in zip(refs[:4], refs[4:8]):
        term = mm_tn(d_ref[...], t_ref[...])
        total = term if total is None else total + term
    out_ref[...] = total.astype(BF16)


def weight_call(pos, sides, pieces, name):
    rows, depth = sides[0].shape
    quarter = depth // 4
    width = pieces[0].shape[1]
    return call(
        weight_body,
        (width // TILE,),
        [
            pl.BlockSpec((rows, quarter), lambda n, pos: (0, pos[1])),
            pl.BlockSpec((rows, quarter), lambda n, pos: (0, lax.rem(pos[1], 2))),
            whole((rows, quarter)),
            whole((rows, quarter)),
        ]
        + [pl.BlockSpec((rows, TILE), lambda n, pos: (0, n))] * 4,
        [(pl.BlockSpec((quarter, TILE), lambda n, pos: (0, n)), sds((quarter, width), BF16))],
        (pos, *sides, *pieces),
        flops=8 * rows * quarter * width,
        moved=8 * rows * width,
        name=name,
    )[0]


def total_body(groups, src, out, here, there, send, recv):
    axes = [name for name, _ in groups]
    index = {name: lax.axis_index(name) for name in axes}
    greet([{name: lax.rem(index[name] + r, n)} for name, n in groups for r in range(1, n)])
    base = 0
    for stage, ((name, n), slots) in enumerate(zip(groups, (here, there))):
        me = index[name]
        value = src[...] if stage == 0 else out[...]
        slots[me] = value
        copies = []
        for r in range(1, n):
            copies.append(
                pltpu.make_async_remote_copy(
                    src_ref=src if stage == 0 else out,
                    dst_ref=slots.at[me],
                    send_sem=send.at[base + r - 1],
                    recv_sem=recv.at[base + r - 1],
                    device_id={name: lax.rem(me + r, n)},
                    device_id_type=MESH,
                )
            )
        for copy in copies:
            copy.start()
        for copy in copies:
            copy.wait()
        base += n - 1
        total = slots[0]
        for i in range(1, n):
            total = total + slots[i]
        out[...] = total


def total_call(groups, values, collective):
    count = sum(n - 1 for _, n in groups)
    return pl.pallas_call(
        functools.partial(total_body, groups),
        out_shape=sds(values.shape, F32),
        in_specs=[VMEM_WHOLE],
        out_specs=VMEM_WHOLE,
        scratch_shapes=[pltpu.VMEM((n, *values.shape), F32) for _, n in groups]
        + [pltpu.SemaphoreType.DMA((count,))] * 2,
        compiler_params=pltpu.CompilerParams(collective_id=collective, has_side_effects=True),
        name="totals",
    )(values)


def swap(values, axis, bit, size):
    return lax.ppermute(values, axis, [(i, i ^ bit) for i in range(size)])


def quick(
    block_input,
    gain_first,
    shift_first,
    attend_weight,
    attend_offset,
    merge_weight,
    merge_offset,
    gain_second,
    shift_second,
    expand_weight,
    expand_offset,
    reduce_weight,
    reduce_offset,
    key_mask,
    true_lengths,
    output_cotangent,
):
    rows, depth = block_input.shape[1:]
    width = merge_weight.shape[0]
    hidden_width = expand_weight.shape[1]
    n = lax.axis_size("context")
    side, batch, place = (lax.axis_index(name) for name in ("tensor", "batch", "context"))
    pos = jnp.stack([side, batch, place]).astype(jnp.int32)
    core, high = lax.rem(batch, 2), batch // 2

    def line(values):
        return values.reshape(1, -1)

    def across(values):
        return swap(values, "tensor", 1, 2)

    def over_y(values):
        return swap(values, "batch", 2, 4)

    def over_core(values):
        return swap(values, "batch", 1, 4)

    def share_sides(values):
        half, quarter = depth // 2, depth // 4
        far = over_y(lax.dynamic_slice(values, (0, (1 - high) * half), (rows, half)))
        near = over_core(lax.dynamic_slice(values, (0, (batch + 1 - 2 * core) * quarter), (rows, quarter)))
        both = over_core(lax.dynamic_slice(far, (0, (1 - core) * quarter), (rows, quarter)))
        return values, far, near, both

    def share_pieces(values):
        far = over_y(values)
        return values, far, over_core(values), over_core(far)

    x = block_input[0]
    half_rows = width // 2
    near_rows = across(lax.dynamic_slice(merge_weight, (core * half_rows, 0), (half_rows, depth)))
    far_rows = over_core(near_rows)

    position = place * rows + jnp.arange(rows, dtype=jnp.int32)
    live = position < true_lengths[0]
    up = jnp.where(live[:, None], output_cotangent[0], jnp.zeros_like(output_cotangent[0]))
    reduce_off_grad = jnp.sum(up.astype(F32), 0)
    flags = jnp.broadcast_to(((key_mask[0] == 1) & live).astype(F32)[None, :], (8, rows))

    weight_three = jnp.transpose(attend_weight, (1, 0, 2))
    qkv, normed = qkv_call(pos, x, line(gain_first), line(shift_first), weight_three, attend_offset)
    heads, all_flags = spread(n, qkv, flags, 1)
    mixed_heads, lse = attend_call(n, pos, heads, all_flags)
    mixed_full, mixed = mixed_call(n, mixed_heads, 2)
    middle, normed_two = merge_call(
        pos, x, mixed_full, merge_weight, near_rows, far_rows, line(merge_offset), line(gain_second), line(shift_second)
    )
    up_sides = share_sides(up)
    normed_sides = share_sides(normed)
    mixed_pieces = share_pieces(mixed)
    normed_two_sides = share_sides(normed_two)

    parts = 2
    actives, hidden_grads, hidden_sums = zip(
        *[
            expand_call(pos, k, parts, normed_two, expand_weight, line(expand_offset), up, reduce_weight)
            for k in range(parts)
        ]
    )
    active_pieces = [share_pieces(values) for values in actives]
    hidden_pieces = [share_pieces(values) for values in hidden_grads]

    second_own = rows_call(pos, hidden_grads, expand_weight, "second_part")
    second_peer = across(second_own)
    reduced_own = columns_call(pos, actives, reduce_weight, "reduced_part")
    reduced_peer = across(reduced_own)
    block_output = (
        middle + (reduced_own.astype(F32) + reduced_peer.astype(F32)) + reduce_offset
    ).astype(BF16)

    mixed_grad, middle_grad, middle_low, gain_two_grad, shift_two_grad, merge_off_grad = middle_back_call(
        pos, second_own, second_peer, middle, line(gain_second), up, merge_weight
    )
    mixed_grad_heads = spread(n, mixed_grad[None], None, 3)[0]
    triple_heads = attend_back_call(n, pos, heads, all_flags, lse, mixed_grad_heads[0])
    triple = collect(n, triple_heads, 4)
    first_own, offset_grad = first_call(pos, triple, weight_three)
    first_peer = across(first_own)
    input_gradient, gain_one_grad, shift_one_grad = input_back_call(
        first_own, first_peer, x, line(gain_first), middle_grad
    )

    def scatter(values, axis=0):
        return lax.psum_scatter(values, "context", scatter_dimension=axis, tiled=True)

    reduce_total = jnp.concatenate(
        [
            scatter(weight_call(pos, up_sides, pieces, f"reduce_grad{k}")).T.astype(F32)
            for k, pieces in enumerate(active_pieces)
        ],
        axis=0,
    )
    expand_total = jnp.concatenate(
        [
            scatter(weight_call(pos, normed_two_sides, pieces, f"expand_grad{k}")).astype(F32)
            for k, pieces in enumerate(hidden_pieces)
        ],
        axis=1,
    )
    middle_sides = share_sides(middle_low)
    merge_total = scatter(weight_call(pos, middle_sides, mixed_pieces, "merge_grad")).T.astype(F32)
    attend_total = jnp.stack(
        [
            scatter(weight_call(pos, normed_sides, share_pieces(triple[c]), f"attend_grad{c}")).astype(F32)
            for c in range(3)
        ],
        axis=1,
    )

    smalls = [
        gain_one_grad,
        shift_one_grad,
        offset_grad,
        merge_off_grad,
        gain_two_grad,
        shift_two_grad,
        *hidden_sums,
        reduce_off_grad,
    ]
    flat = jnp.concatenate([values.reshape(-1) for values in smalls]).reshape(-1, 128)
    totals = total_call((("batch", 4), ("context", n)), flat, 5).reshape(-1)
    sizes = [depth, depth, 2 * width, depth, depth, depth, hidden_width, depth]
    starts = [sum(sizes[:i]) for i in range(len(sizes))]
    gain_one, shift_one, offset, merge_off, gain_two, shift_two, expand_off, reduce_off = (
        totals[start : start + size] for start, size in zip(starts, sizes)
    )
    return (
        block_output[None],
        input_gradient[None],
        gain_one,
        shift_one,
        attend_total,
        offset.reshape(2, width),
        merge_total,
        merge_off,
        gain_two,
        shift_two,
        expand_total,
        expand_off,
        reduce_total,
        reduce_off,
    )


def local(*operands):
    heads = operands[3].shape[2] // HEAD_DIM
    fits = lax.axis_size("tensor") == 2 and lax.axis_size("batch") == 4 and heads % lax.axis_size("context") == 0
    return (quick if fits else general)(*operands)


def solution(mesh):
    return jax.shard_map(
        local,
        mesh=mesh,
        in_specs=(
            P("batch", "context", None),
            P(),
            P(),
            P(None, None, "tensor"),
            P(None, "tensor"),
            P("tensor", None),
            P(),
            P(),
            P(),
            P(None, "tensor"),
            P("tensor"),
            P("tensor", None),
            P(),
            P("batch", "context"),
            P("batch"),
            P("batch", "context", None),
        ),
        out_specs=(
            P("batch", "context", None),
            P("batch", "context", None),
            P(),
            P(),
            P(("batch", "context"), None, "tensor"),
            P(None, "tensor"),
            P("tensor", ("batch", "context")),
            P(),
            P(),
            P(),
            P(("batch", "context"), "tensor"),
            P("tensor"),
            P("tensor", ("batch", "context")),
            P(),
        ),
        check_vma=False,
    )
```
